32 devices in a mesh: dp: 2 (over z, core), ep: 16 (over x, y).
Axes of the slice: x: 4, y: 4, z: 1, core: 2. Of those that a mesh axis runs over, the one named last changes fastest.
The devices are a block of a 4x4x8 slice.
Arguments:
- x: bfloat16 [2, 16, 256, 4096], P('dp', 'ep'), parts along dimension 0
- expert: int32 [2, 16, 256, 8], P('dp', 'ep'), parts along dimension 0
- slot: int32 [2, 16, 256, 8], P('dp', 'ep'), parts along dimension 0
- gate: float32 [2, 16, 256, 8], P('dp', 'ep'), parts along dimension 0
- w_gate: bfloat16 [64, 4096, 1536], P('ep')
- w_up: bfloat16 [64, 4096, 1536], P('ep')
- w_down: bfloat16 [64, 1536, 4096], P('ep')
Outputs:
- y: bfloat16 [2, 16, 256, 4096], P('dp', 'ep'), parts along dimension 0
There are 2 independent parts. The reference program is written for one: setup_inputs(seed, part) draws one part's arguments, and reference() takes and returns one part's arrays. A program takes and returns all parts, laid end to end along the dimension named above; an argument that names none is the same for every part.
All inputs are finite; a program needn't handle non-finite values.
Results may differ from the reference program's by a relative error of at most 0.009.
Values are sent between devices in bfloat16 or wider.
A program may use at most 768 MiB of HBM per device.

```python
import jax
import jax.numpy as jnp

MEMBERS = 16
TOKENS = 256
D = 4096
FF = 1536
TOP = 8
EXPERTS = 64
SLOTS = 5 * TOKENS * TOP // (4 * EXPERTS)


def setup_inputs(seed: int = 0, part: int = 0) -> dict:
    own, k1, k2, k3, k4, k5, k6 = jax.random.split(jax.random.key(seed), 7)
    kx, ke, kl, kg = jax.random.split(jax.random.fold_in(own, part), 4)
    devices = (1, MEMBERS)
    place = jax.random.permutation(kl, jnp.arange(EXPERTS, dtype=jnp.uint32))
    slow = ((EXPERTS + (9 * place) % EXPERTS) << ((9 * place) // EXPERTS)) // EXPERTS
    wait = (jax.random.bits(ke, (*devices, TOKENS, EXPERTS), jnp.uint32) >> 10) * slow
    expert = jnp.argsort(wait, axis=-1)[..., :TOP].astype(jnp.int32)
    chosen = jax.nn.one_hot(expert, EXPERTS, dtype=jnp.int32)
    in_line = jnp.cumsum(chosen.reshape(*devices, TOKENS * TOP, EXPERTS), axis=2) - 1
    slot = jnp.sum(in_line.reshape(chosen.shape) * chosen, axis=-1)

    def one(key, rows, columns):
        return (jax.random.normal(key, (rows, columns), jnp.float32) * rows**-0.5).astype(jnp.bfloat16)

    def weights(key, rows, columns):
        return jax.lax.map(lambda k: one(k, rows, columns), jax.random.split(key, EXPERTS))

    return {
        "x": jax.random.normal(kx, (*devices, TOKENS, D), jnp.float32).astype(jnp.bfloat16),
        "expert": expert,
        "slot": slot,
        "gate": jax.nn.softmax(jax.random.normal(kg, expert.shape, jnp.float32)),
        "w_gate": weights(k1, D, FF),
        "w_up": weights(k2, D, FF),
        "w_down": weights(k3, FF, D),
    }


def einsum(form, a, b):
    return jnp.einsum(form, a.astype(jnp.float32), b.astype(jnp.float32))


def reference(x, expert, slot, gate, w_gate, w_up, w_down):
    to_expert = jax.nn.one_hot(expert, EXPERTS, dtype=jnp.bfloat16)
    to_slot = jax.nn.one_hot(slot, SLOTS, dtype=jnp.bfloat16)
    weighted = to_expert * gate[..., None].astype(jnp.bfloat16)
    dispatch = einsum("abtke,abtkc->abtec", to_expert, to_slot).astype(jnp.bfloat16)
    combine = einsum("abtke,abtkc->abtec", weighted, to_slot).astype(jnp.bfloat16)
    z = einsum("abtec,abtd->aebcd", dispatch, x).astype(jnp.bfloat16)
    h = jax.nn.silu(einsum("aebcd,edf->aebcf", z, w_gate))
    h = (h * einsum("aebcd,edf->aebcf", z, w_up)).astype(jnp.bfloat16)
    out = einsum("aebcf,efd->aebcd", h, w_down).astype(jnp.bfloat16)
    y = einsum("abtec,aebcd->abtd", combine, out)
    return y.astype(jnp.bfloat16)
```

```python
import functools
import math

import jax
import jax.numpy as jnp
from jax import lax
from jax.experimental import pallas as pl
from jax.experimental.pallas import tpu as pltpu
from jax.sharding import PartitionSpec as P

F32, BF16 = jnp.float32, jnp.bfloat16
WIDE_IN = 1024
WIDE_OUT = 512
VMEM = 66_900_000


class Torus:
    def __init__(self, side):
        self.side = side
        self.me = lax.axis_index("ep")
        self.at = (self.me // side, self.me % side)

    def step(self, axis, by):
        return (self.at[axis] + by + self.side) % self.side

    def near(self, axis, by):
        place = list(self.at)
        place[axis] = self.step(axis, by)
        return place[0] * self.side + place[1]


def send(src, dst, sems, device):
    return pltpu.make_async_remote_copy(
        src_ref=src, dst_ref=dst, send_sem=sems[0], recv_sem=sems[1],
        device_id={"ep": device}, device_id_type=pl.DeviceIdType.MESH)


def greet(devices):
    barrier = pltpu.get_barrier_semaphore()
    for d in devices:
        pl.semaphore_signal(barrier, inc=1, device_id={"ep": d}, device_id_type=pl.DeviceIdType.MESH)
    pl.semaphore_wait(barrier, len(devices))


def gather_kernel(side, pairs, top, slots, meta_ref, row_ref, x_ref, wg_ref, wu_ref, h_ref, w2_ref, xall,
                  acc_g, acc_u, xv, xb, z, d2, stage, meta, ssem, rsem, msend, mrecv, lsem, bsem, wsem):
    p, e = pl.program_id(0), pl.program_id(1)
    experts = pl.num_programs(1)
    n = side * side
    tokens, hw = xv.shape[1:]
    half = tokens // 2
    torus = Torus(side)
    me, (cx, cy) = torus.me, torus.at
    halves = (pl.ds(0, half), pl.ds(half, half))

    def block(c, axis, by):
        place = list(torus.at)
        place[axis] = torus.step(axis, by)
        return xall.at[c, place[0], place[1]]

    def line(c, t, by):
        if t == 0:
            return xall.at[c, :, torus.step(1, by)]
        return xall.at[c, torus.step(0, by)]

    def line_half(c, t, by, d):
        if t == 0:
            return xall.at[c, :, torus.step(1, by), halves[d]]
        return xall.at[c, torus.step(0, by), :, halves[d]]

    def sems(stage, c, d):
        return ssem.at[stage, c, d], rsem.at[stage, c, d]

    def first(c, t, d):
        return send(xv.at[c], block(c, t, 0), sems(0, c, d), torus.near(t, 1 - 2 * d))

    def first_got(c, t, d):
        b = block(c, t, 2 * d - 1)
        return send(b, b, sems(0, c, d), torus.near(t, 1 - 2 * d))

    def first_on(c, t, d):
        b = block(c, t, 2 * d - 1).at[halves[d]]
        return send(b, b, sems(1, c, d), torus.near(t, 1 - 2 * d))

    def first_on_got(c, t, d):
        b = block(c, t, 2).at[halves[d]]
        return send(b, b, sems(1, c, d), torus.near(t, 1 - 2 * d))

    def second(c, t, d):
        b = line(c, t, 0)
        return send(b, b, sems(2, c, d), torus.near(1 - t, 1 - 2 * d))

    def second_got(c, t, d):
        b = line(c, t, 2 * d - 1)
        return send(b, b, sems(2, c, d), torus.near(1 - t, 1 - 2 * d))

    def second_on(c, t, d):
        b = line_half(c, t, 2 * d - 1, d)
        return send(b, b, sems(3, c, d), torus.near(1 - t, 1 - 2 * d))

    def second_on_got(c, t, d):
        b = line_half(c, t, 2, d)
        return send(b, b, sems(3, c, d), torus.near(1 - t, 1 - 2 * d))

    ways = [(t, d) for t in range(2) for d in range(2)]

    def start_second(q):
        for t, d in ways:
            first_on_got(2 * q + t, t, d).wait_recv()
        for t, d in ways:
            second(2 * q + t, t, d).start()

    def pass_second(q):
        for t, d in ways:
            second_got(2 * q + t, t, d).wait_recv()
        for t, d in ways:
            second_on(2 * q + t, t, d).start()

    def own_copy(c):
        return pltpu.make_async_copy(xv.at[c], xall.at[c, cx, cy], lsem.at[c])

    @pl.when((p == 0) & (e == 0))
    def _():
        loads = [pltpu.make_async_copy(x_ref.at[:, pl.ds(c * hw, hw)], xv.at[c], lsem.at[c])
                 for c in range(2 * pairs)]
        for copy in loads:
            copy.start()
        greet([lax.rem(me + d, n) for d in range(1, n)])
        for c in range(2 * pairs):
            loads[c].wait()
            for d in range(2):
                first(c, c % 2, d).start()
        for c in range(2 * pairs):
            own_copy(c).start()

        def tell(d):
            return send(meta_ref, meta.at[me], (msend.at[d], mrecv.at[d]), lax.rem(me + d, n))

        def told(d):
            ref = meta.at[lax.rem(me + n - d, n)]
            return send(ref, ref, (msend.at[d], mrecv.at[d]), lax.rem(me + d, n))

        for d in range(1, n):
            tell(d).start()
        meta[me] = meta_ref[...]
        for c in range(2 * pairs):
            for d in range(2):
                first_got(c, c % 2, d).wait_recv()
                first_on(c, c % 2, d).start()
        for c in range(2 * pairs):
            own_copy(c).wait()
        for q in range(min(2, pairs)):
            start_second(q)
        for d in range(1, n):
            told(d).wait_recv()

        @pl.loop(0, n // 2)
        def _(q):
            m0, m1 = meta[2 * q], meta[2 * q + 1]
            other = jnp.float32(2 * n * experts * slots)
            code = jnp.concatenate([m0[:top], m1[:top] + other], axis=1)
            gate = jnp.concatenate([m0[top:], m1[top:]], axis=1)
            row = row_ref[:, :1]
            hot = jnp.zeros((row.shape[0], 2 * tokens), F32)
            weight = jnp.zeros((row.shape[0], 2 * tokens), F32)
            for j in range(top):
                hit = code[j:j + 1] == row
                hot = jnp.where(hit, 1.0, hot)
                weight = jnp.where(hit, gate[j:j + 1], weight)
            d2[q] = hot.astype(BF16)
            stage[...] = weight.T.astype(BF16)
            out = pltpu.make_async_copy(stage, w2_ref.at[q], wsem)
            out.start()
            out.wait()

        pass_second(0)
        if pairs > 2:
            start_second(2)

    @pl.when(e == 0)
    def _():
        @pl.when(p + 1 < pairs)
        def _():
            pass_second(p + 1)

        @pl.when(p + 3 < pairs)
        def _():
            start_second(p + 3)

        for t, d in ways:
            second_on_got(2 * p + t, t, d).wait_recv()

        def fetch(q, slot):
            s = q * 2
            return [pltpu.make_async_copy(
                xall.at[2 * p + t, s // side, pl.ds(s % side, 2)], xb.at[slot, t], bsem.at[slot, t])
                for t in range(2)]

        for copy in fetch(0, 0):
            copy.start()

        @pl.loop(0, n // 2)
        def _(q):
            slot = lax.rem(q, 2)
            for copy in fetch(q, slot):
                copy.wait()

            @pl.when(q + 1 < n // 2)
            def _():
                for copy in fetch(q + 1, 1 - slot):
                    copy.start()

            for t in range(2):
                got = jnp.dot(d2[q], xb[slot, t].reshape(2 * tokens, hw), preferred_element_type=F32).astype(BF16)
                for k in range(z.shape[0]):
                    z[k, pl.ds(pl.multiple_of(q * 2 * slots, 2 * slots), 2 * slots), pl.ds(t * hw, hw)] = (
                        got[k * 2 * slots:(k + 1) * 2 * slots])

    ff = wg_ref.shape[2]
    tile = math.gcd(ff, 512)
    for o in range(0, ff, tile):
        cols = pl.ds(o, tile)
        g = jnp.dot(z[e], wg_ref[0, :, cols], preferred_element_type=F32)
        u = jnp.dot(z[e], wu_ref[0, :, cols], preferred_element_type=F32)

        @pl.when(p == 0)
        def _():
            acc_g[e, :, cols] = g
            acc_u[e, :, cols] = u

        @pl.when((p > 0) & (p < pairs - 1))
        def _():
            acc_g[e, :, cols] += g
            acc_u[e, :, cols] += u

        @pl.when(p == pairs - 1)
        def _():
            whole = acc_g[e, :, cols] + g
            h_ref[0, :, cols] = (jax.nn.silu(whole) * (acc_u[e, :, cols] + u)).astype(BF16)

    @pl.when((p == pairs - 1) & (e == experts - 1))
    def _():
        for c in range(2 * pairs):
            for d in range(2):
                t = c % 2
                first(c, t, d).wait_send()
                first_on(c, t, d).wait_send()
                second(c, t, d).wait_send()
                second_on(c, t, d).wait_send()
        for d in range(1, n):
            ref = meta.at[me]
            send(meta_ref, ref, (msend.at[d], mrecv.at[d]), lax.rem(me + d, n)).wait_send()


def scatter_kernel(side, pairs, slots, h_ref, wd_ref, w2_hbm, y_ref,
                   w2, o, part, keep, sh1, sf1, sh2, sf2, rh1, rf1, rh2, rf2, ssem, rsem, wsem):
    p, e = pl.program_id(0), pl.program_id(1)
    experts = pl.num_programs(1)
    n = side * side
    tokens, hw = part.shape[-2:]
    half = tokens // 2
    torus = Torus(side)
    halves = (pl.ds(0, half), pl.ds(half, half))
    ways = [(t, d) for t in range(2) for d in range(2)]
    staged, landed = (sh1, sf1, sh2, sf2), (rh1, rf1, rh2, rf2)

    def first_axis(t):
        return 1 - t

    def copy(stage, i, t, d):
        axis = first_axis(t) if stage < 2 else t
        return send(staged[stage].at[lax.rem(i, 2), t, d], landed[stage].at[lax.rem(i, 3), t, d],
                    (ssem.at[stage, lax.rem(i, 2), t, d], rsem.at[stage, lax.rem(i, 3), t, d]),
                    torus.near(axis, 1 - 2 * d))

    def free(stage, i):
        @pl.when(i >= 2)
        def _():
            for t, d in ways:
                copy(stage, i - 2, t, d).wait_send()

    def go(stage, i):
        for t, d in ways:
            copy(stage, i, t, d).start()

    def got(stage, i):
        for t, d in ways:
            copy(stage, i, t, d).wait_recv()

    def piece(i, t, by, j):
        g = torus.step(first_axis(t), by)
        return part.at[lax.rem(i, 2), t, j, g] if t == 0 else part.at[lax.rem(i, 2), t, g, j]

    @pl.when((p == 0) & (e == 0))
    def _():
        load = pltpu.make_async_copy(w2_hbm, w2, wsem)
        load.start()
        greet([torus.near(axis, by) for axis in range(2) for by in (1, -1)])
        load.wait()

    @pl.when(p < pairs)
    def _():
        tall = h_ref.shape[1]
        out = jnp.dot(h_ref[0], wd_ref[0], preferred_element_type=F32).astype(BF16)
        rows = pl.ds(pl.multiple_of(e * 2 * slots, 2 * slots), 2 * slots)
        for q in range(tall // (2 * slots)):
            o[q, rows] = out[q * 2 * slots:(q + 1) * 2 * slots]

    @pl.when((p < pairs) & (e == experts - 1))
    def _():
        @pl.loop(0, n // 2)
        def _(q):
            s = 2 * q
            both = jnp.dot(w2[q], o[q], preferred_element_type=F32)
            for k in range(2):
                for t in range(2):
                    part[lax.rem(p, 2), t, s // side, s % side + k] = (
                        both[k * tokens:(k + 1) * tokens, t * hw:(t + 1) * hw])

        free(0, p)
        for t, d in ways:
            @pl.loop(0, side)
            def _(j):
                sh1[lax.rem(p, 2), t, d, j] = piece(p, t, 2, j)[halves[d], :].astype(BF16)
        go(0, p)

    @pl.when((e == experts - 1) & (p >= 1) & (p < pairs + 1))
    def _():
        i = p - 1
        got(0, i)
        free(1, i)
        for t, d in ways:
            @pl.loop(0, side)
            def _(j):
                mine = piece(i, t, 1 - 2 * d, j)
                there = rh1[lax.rem(i, 3), t, d, j].astype(F32)
                sf1[lax.rem(i, 2), t, d, j, halves[d]] = (mine[halves[d], :] + there).astype(BF16)
                sf1[lax.rem(i, 2), t, d, j, halves[1 - d]] = mine[halves[1 - d], :].astype(BF16)
        go(1, i)
        for t in range(2):
            @pl.loop(0, side)
            def _(j):
                keep[lax.rem(i, 4), t, j] = piece(i, t, 0, j)[...]

    @pl.when((e == experts - 1) & (p >= 2) & (p < pairs + 2))
    def _():
        i = p - 2
        got(1, i)
        free(2, i)
        for t in range(2):
            @pl.loop(0, side)
            def _(j):
                keep[lax.rem(i, 4), t, j] = (keep[lax.rem(i, 4), t, j] + rf1[lax.rem(i, 3), t, 0, j].astype(F32)
                                             + rf1[lax.rem(i, 3), t, 1, j].astype(F32))
        for t, d in ways:
            far = keep.at[lax.rem(i, 4), t, torus.step(t, 2)]
            sh2[lax.rem(i, 2), t, d] = far[halves[d], :].astype(BF16)
        go(2, i)

    @pl.when((e == experts - 1) & (p >= 3) & (p < pairs + 3))
    def _():
        i = p - 3
        got(2, i)
        free(3, i)
        for t, d in ways:
            mine = keep.at[lax.rem(i, 4), t, torus.step(t, 1 - 2 * d)]
            there = rh2[lax.rem(i, 3), t, d].astype(F32)
            sf2[lax.rem(i, 2), t, d, halves[d]] = (mine[halves[d], :] + there).astype(BF16)
            sf2[lax.rem(i, 2), t, d, halves[1 - d]] = mine[halves[1 - d], :].astype(BF16)
        go(3, i)

    @pl.when((e == experts - 1) & (p >= 4))
    def _():
        i = p - 4
        got(3, i)
        for t in range(2):
            y_ref[:, pl.ds(t * hw, hw)] = (
                keep[lax.rem(i, 4), t, torus.at[t]] + rf2[lax.rem(i, 3), t, 0].astype(F32)
                + rf2[lax.rem(i, 3), t, 1].astype(F32)).astype(y_ref.dtype)

    @pl.when((e == experts - 1) & (p == pairs + 3))
    def _():
        for stage in range(4):
            for i in range(max(0, pairs - 2), pairs):
                for t, d in ways:
                    copy(stage, jnp.int32(i), t, d).wait_send()


def solution(mesh, wide_in=WIDE_IN, wide_out=WIDE_OUT, limit=VMEM):
    n = mesh.shape["ep"]
    side = math.isqrt(n)
    dma = pltpu.SemaphoreType.DMA

    def step(x, expert, slot, gate, wg, wu, wd):
        x, expert, slot, gate = x[0, 0], expert[0, 0], slot[0, 0], gate[0, 0]
        tokens, d = x.shape
        top = expert.shape[1]
        local, _, ff = wg.shape
        slots = 5 * tokens * top // (4 * local * n)
        rows = local * 2 * slots
        tall = n * slots
        big = n * local * slots
        code = jnp.where(slot < slots, expert * slots + slot, -4 * big).astype(F32)
        meta = jnp.concatenate([code.T, gate.T], axis=0)
        me = lax.axis_index("ep")
        r = jnp.arange(rows, dtype=jnp.int32)
        kind = (me * local + r // (2 * slots)) * slots + r % slots + (r // slots % 2) * 2 * big
        kind = jnp.broadcast_to(kind.astype(F32)[:, None], (rows, 128))

        pairs, hw = d // wide_in, wide_in // 2
        any_ = pl.BlockSpec(memory_space=pl.ANY)
        weight = pl.BlockSpec((1, wide_in, ff), lambda p, e: (e, p, 0))
        h, w2, _ = pl.pallas_call(
            functools.partial(gather_kernel, side, pairs, top, slots),
            grid=(pairs, local),
            in_specs=[pl.BlockSpec((2 * top, tokens), lambda p, e: (0, 0)),
                      pl.BlockSpec((rows, 128), lambda p, e: (0, 0)), any_, weight, weight],
            out_specs=[pl.BlockSpec((1, tall, ff), lambda p, e: (jnp.where(p == pairs - 1, e, 0), 0, 0)),
                       any_, any_],
            out_shape=[jax.ShapeDtypeStruct((local, tall, ff), BF16),
                       jax.ShapeDtypeStruct((n // 2, 2 * tokens, rows), BF16),
                       jax.ShapeDtypeStruct((2 * pairs, side, side, tokens, hw), BF16)],
            scratch_shapes=[
                pltpu.VMEM((local, tall, ff), F32), pltpu.VMEM((local, tall, ff), F32),
                pltpu.VMEM((2 * pairs, tokens, hw), BF16),
                pltpu.VMEM((2, 2, 2, tokens, hw), BF16),
                pltpu.VMEM((local, tall, wide_in), BF16),
                pltpu.VMEM((n // 2, rows, 2 * tokens), BF16),
                pltpu.VMEM((2 * tokens, rows), BF16),
                pltpu.VMEM((n, 2 * top, tokens), F32),
                dma((4, 2 * pairs, 2)), dma((4, 2 * pairs, 2)), dma((n,)), dma((n,)),
                dma((2 * pairs,)), dma((2, 2)), dma],
            compiler_params=pltpu.CompilerParams(
                collective_id=0, has_side_effects=True, vmem_limit_bytes=limit,
                dimension_semantics=("arbitrary", "arbitrary")),
        )(meta, kind, x, wg, wu)

        pairs, hw = d // wide_out, wide_out // 2
        half = tokens // 2
        y = pl.pallas_call(
            functools.partial(scatter_kernel, side, pairs, slots),
            grid=(pairs + 4, local),
            in_specs=[pl.BlockSpec((1, tall, ff), lambda p, e: (jnp.where(p < pairs, e, local - 1), 0, 0)),
                      pl.BlockSpec((1, ff, wide_out), lambda p, e: (
                          jnp.where(p < pairs, e, local - 1), 0, jnp.minimum(p, pairs - 1))), any_],
            out_specs=pl.BlockSpec((tokens, wide_out), lambda p, e: (0, jnp.maximum(p - 4, 0))),
            out_shape=jax.ShapeDtypeStruct((tokens, d), BF16),
            scratch_shapes=[
                pltpu.VMEM((n // 2, 2 * tokens, rows), BF16),
                pltpu.VMEM((n // 2, rows, wide_out), BF16),
                pltpu.VMEM((2, 2, side, side, tokens, hw), F32),
                pltpu.VMEM((4, 2, side, tokens, hw), F32),
                pltpu.VMEM((2, 2, 2, side, half, hw), BF16), pltpu.VMEM((2, 2, 2, side, tokens, hw), BF16),
                pltpu.VMEM((2, 2, 2, half, hw), BF16), pltpu.VMEM((2, 2, 2, tokens, hw), BF16),
                pltpu.VMEM((3, 2, 2, side, half, hw), BF16), pltpu.VMEM((3, 2, 2, side, tokens, hw), BF16),
                pltpu.VMEM((3, 2, 2, half, hw), BF16), pltpu.VMEM((3, 2, 2, tokens, hw), BF16),
                dma((4, 2, 2, 2)), dma((4, 3, 2, 2)), dma],
            compiler_params=pltpu.CompilerParams(
                collective_id=1, has_side_effects=True, vmem_limit_bytes=limit,
                dimension_semantics=("arbitrary", "arbitrary")),
        )(h, wd, w2)
        return y[None, None]

    return jax.shard_map(
        step, mesh=mesh, in_specs=(P("dp", "ep"),) * 4 + (P("ep"),) * 3,
        out_specs=P("dp", "ep"), check_vma=False)
```

```python
import functools
import math

import jax
import jax.numpy as jnp
from jax import lax
from jax.experimental import pallas as pl
from jax.experimental.pallas import tpu as pltpu
from jax.sharding import PartitionSpec as P

F32, BF16 = jnp.float32, jnp.bfloat16
WIDE_IN = 512
WIDE_OUT = 512
VMEM = 66_900_000


class Torus:
    def __init__(self, side):
        self.side = side
        self.me = lax.axis_index("ep")
        self.at = (self.me // side, self.me % side)

    def step(self, axis, by):
        return (self.at[axis] + by + self.side) % self.side

    def near(self, axis, by):
        place = list(self.at)
        place[axis] = self.step(axis, by)
        return place[0] * self.side + place[1]


def send(src, dst, sems, device):
    return pltpu.make_async_remote_copy(
        src_ref=src, dst_ref=dst, send_sem=sems[0], recv_sem=sems[1],
        device_id={"ep": device}, device_id_type=pl.DeviceIdType.MESH)


def greet(devices):
    barrier = pltpu.get_barrier_semaphore()
    for d in devices:
        pl.semaphore_signal(barrier, inc=1, device_id={"ep": d}, device_id_type=pl.DeviceIdType.MESH)
    pl.semaphore_wait(barrier, len(devices))


def spot(torus, t, j):
    return torus.at[0] * torus.side + j if t == 0 else j * torus.side + torus.at[1]


def gather_kernel(side, chunks, top, slots, meta_ref, row_ref, row2_ref, x_ref, wg_ref, wu_ref,
                  h_ref, w2_ref, zall, relay,
                  acc_g, acc_u, xl, zb, zs, d2, stage, meta,
                  ssem, rsem, msend, mrecv, lsem, zsem, osem, hsem, wsem):
    c, e = pl.program_id(0), pl.program_id(1)
    experts = pl.num_programs(1)
    local = zb.shape[0]
    tokens, hw = xl.shape[2:]
    torus = Torus(side)
    at = torus.at
    halves = (pl.ds(0, tokens // 2), pl.ds(tokens // 2, tokens // 2))
    parts = (pl.ds(0, local // 2), pl.ds(local // 2, local // 2))
    depth = zs.shape[0]
    step_of, last = c * experts + e, chunks - 1

    def sems(stage, k, d):
        return ssem.at[stage, k, d], rsem.at[stage, k, d]

    def first(k, t, d, by):
        b = xl.at[k, torus.step(t, by)]
        return send(b, b, sems(0, k, d), torus.near(t, 1 - 2 * d))

    def first_on(k, t, d, by):
        b = xl.at[k, torus.step(t, by), halves[d]]
        return send(b, b, sems(1, k, d), torus.near(t, 1 - 2 * d))

    def whole(k, t, d, by):
        return send(zs.at[lax.rem(k, depth), torus.step(1 - t, 1 - 2 * d)], zall.at[k, :, torus.step(1 - t, by)],
                    sems(2, k, d), torus.near(1 - t, 1 - 2 * d))

    def hop(k, t, d):
        return send(zs.at[lax.rem(k, depth), torus.step(1 - t, 2), parts[d]], relay.at[k, d],
                    sems(3, k, d), torus.near(1 - t, 1 - 2 * d))

    def hop_on(k, t, d, by):
        return send(relay.at[k, d], zall.at[k, parts[d], torus.step(1 - t, by)],
                    sems(4, k, d), torus.near(1 - t, 1 - 2 * d))

    def own(k, t):
        return pltpu.make_async_copy(zs.at[lax.rem(k, depth), at[1 - t]], zall.at[k, :, at[1 - t]],
                                     osem.at[lax.rem(k, depth)])

    def tell(axis, by, where):
        return send(meta_ref, meta.at[axis, torus.step(axis, where)],
                    (msend.at[axis, by], mrecv.at[axis, by]), torus.near(axis, by))

    def dispatch(k, t):
        slot = lax.rem(k, depth)
        for d in range(2):
            first_on(k, t, d, 2).wait_recv()

        @pl.when(k >= depth)
        def _():
            for d in range(2):
                hop(k - depth, t, d).wait_send()
                whole(k - depth, t, d, 0).wait_send()

        @pl.loop(0, side)
        def _(j):
            for q in range(side // 2):
                got = [jnp.dot(d2[t, j, 2 * q + i], xl[k, 2 * q + i], preferred_element_type=F32) for i in range(2)]
                for m in range(local):
                    rows = slice(m * slots, (m + 1) * slots)
                    zs[slot, j, m, q * 2 * slots:(q + 1) * 2 * slots] = (
                        jnp.concatenate([got[0][rows], got[1][rows]], axis=0).astype(BF16))
        for d in range(2):
            hop(k, t, d).start()
        for d in range(2):
            whole(k, t, d, 0).start()
        own(k, t).start()

    def pass_on(k, t):
        for d in range(2):
            hop(k, t, d).wait_recv()
            hop_on(k, t, d, 2 * d - 1).start()

    @pl.when(step_of == 0)
    def _():
        loads = [pltpu.make_async_copy(x_ref.at[:, pl.ds(k * hw, hw)], xl.at[k, at[k % 2]], lsem.at[k])
                 for k in range(chunks)]
        for copy in loads:
            copy.start()
        greet([torus.near(axis, by) for axis in range(2) for by in range(1, side)])
        for axis in range(2):
            for by in range(1, side):
                tell(axis, by, 0).start()
        for k in range(chunks):
            loads[k].wait()
            for d in range(2):
                first(k, k % 2, d, 0).start()
        for axis in range(2):
            meta[axis, at[axis]] = meta_ref[...]
        for axis in range(2):
            for by in range(1, side):
                tell(axis, by, -by).wait_recv()

        def build(t, i):
            @pl.loop(0, side)
            def _(j):
                code = meta[t, i][:top]
                row = row_ref[:, :1] + (spot(torus, t, j) * local * slots).astype(F32)
                hot = jnp.zeros((row.shape[0], tokens), F32)
                for m in range(top):
                    hot = jnp.where(code[m:m + 1] == row, 1.0, hot)
                d2[t, j, i] = hot.astype(BF16)

        todo = [(t, i) for t in range(2) for i in range(side)]
        for k in range(chunks):
            for d in range(2):
                first(k, k % 2, d, 2 * d - 1).wait_recv()
                first_on(k, k % 2, d, 2 * d - 1).start()
            for t, i in todo[k * len(todo) // chunks:(k + 1) * len(todo) // chunks]:
                build(t, i)
        dispatch(0, 0)
        dispatch(1, 1)
        pass_on(0, 0)
        pass_on(1, 1)
        dispatch(2, 0)

    @pl.when(e == 0)
    def _():
        for t in range(2):
            @pl.when((c + 3 < chunks) & (lax.rem(c, 2) == 1 - t))
            def _():
                dispatch(c + 3, t)

        for t in range(2):
            @pl.when((c + 2 < chunks) & (lax.rem(c, 2) == t))
            def _():
                pass_on(c + 2, t)

            @pl.when(lax.rem(c, 2) == t)
            def _():
                for d in range(2):
                    whole(c, t, d, 2 * d - 1).wait_recv()
                    hop_on(c, t, d, 2).wait_recv()
                own(c, t).wait()
        for m in range(local):
            pltpu.make_async_copy(zall.at[c, m], zb.at[m], zsem.at[m]).start()

    @pl.when((step_of >= 8) & (step_of < 8 + 4 * side))
    def _():
        m = step_of - 8
        t, j, q = m // (2 * side), m // 2 % side, m % 2
        m0, m1 = meta[t, 2 * q], meta[t, 2 * q + 1]
        far = jnp.float32(2 * side * side * local * slots)
        code = jnp.concatenate([m0[:top], m1[:top] + far], axis=1)
        gate = jnp.concatenate([m0[top:], m1[top:]], axis=1)
        device = jnp.where(t == 0, at[0] * side + j, j * side + at[1])
        row = row2_ref[:, :1] + (device * local * slots).astype(F32)
        weight = jnp.zeros((row.shape[0], 2 * tokens), F32)
        for k in range(top):
            weight = jnp.where(code[k:k + 1] == row, gate[k:k + 1], weight)

        @pl.when(m > 0)
        def _():
            pltpu.make_async_copy(stage, w2_ref.at[m - 1], wsem).wait()

        stage[...] = weight.T.astype(BF16)
        pltpu.make_async_copy(stage, w2_ref.at[m], wsem).start()

    pltpu.make_async_copy(zall.at[c, e], zb.at[e], zsem.at[e]).wait()
    rows, ff = acc_g.shape[1:]
    tile = math.gcd(ff, hw)

    def products(o):
        cols = pl.ds(o, tile)
        zed = zb[e].reshape(rows, hw)
        return (cols, jnp.dot(zed, wg_ref[0, :, cols], preferred_element_type=F32),
                jnp.dot(zed, wu_ref[0, :, cols], preferred_element_type=F32))

    @pl.when(c == 0)
    def _():
        for o in range(0, ff, tile):
            cols, g, u = products(o)
            acc_g[e, :, cols] = g
            acc_u[e, :, cols] = u

    @pl.when((c > 0) & (lax.rem(c, 2) == 0))
    def _():
        for o in range(0, ff, tile):
            cols, g, u = products(o)
            acc_g[e, :, cols] += g
            acc_u[e, :, cols] += u

    @pl.when(lax.rem(c, 2) == 1)
    def _():
        for o in range(0, ff, tile):
            cols, g, u = products(o)
            for i in range(side):
                for j in range(side):
                    a, b = (i * side + j) * slots, (j * side + i) * slots
                    acc_g[e, a:a + slots, cols] += g[b:b + slots]
                    acc_u[e, a:a + slots, cols] += u[b:b + slots]

    @pl.when(c == last)
    def _():
        spare = (chunks - depth) % depth

        def put(m, o):
            return pltpu.make_async_copy(zs.at[spare, o // tile, :, :, pl.ds(0, tile)],
                                         h_ref.at[m, :, :, pl.ds(o, tile)], hsem.at[o // tile])

        @pl.when(e == 0)
        def _():
            for d in range(2):
                k, t = chunks - depth, (chunks - depth) % 2
                hop(k, t, d).wait_send()
                whole(k, t, d, 0).wait_send()

        for o in range(0, ff, tile):
            @pl.when(e > 0)
            def _():
                put(e - 1, o).wait()

            cols = pl.ds(o, tile)
            both = (jax.nn.silu(acc_g[e, :, cols]) * acc_u[e, :, cols]).astype(BF16)
            zs[spare, o // tile, :, :, pl.ds(0, tile)] = both.reshape(local, rows // local, tile)
            put(e, o).start()

        @pl.when(e == experts - 1)
        def _():
            for o in range(0, ff, tile):
                put(e, o).wait()

    @pl.when((c == last) & (e == experts - 1))
    def _():
        pltpu.make_async_copy(stage, w2_ref.at[4 * side - 1], wsem).wait()
        for k in range(chunks):
            for d in range(2):
                t = k % 2
                first(k, t, d, 0).wait_send()
                first_on(k, t, d, 2 * d - 1).wait_send()
                if k > chunks - depth:
                    hop(k, t, d).wait_send()
                    whole(k, t, d, 0).wait_send()
                hop_on(k, t, d, 2 * d - 1).wait_send()
        for axis in range(2):
            for by in range(1, side):
                tell(axis, by, 0).wait_send()


def scatter_kernel(side, pairs, slots, h_ref, wd_ref, w2_hbm, y_ref,
                   w2, so, ro, rl, keep, sh2, sf2, rh2, rf2, ssem, rsem, osem, wsem):
    p, e = pl.program_id(0), pl.program_id(1)
    experts = pl.num_programs(1)
    tokens, hw = keep.shape[-2:]
    half = tokens // 2
    torus = Torus(side)
    at = torus.at
    halves = (pl.ds(0, half), pl.ds(half, half))
    ways = [(t, d) for t in range(2) for d in range(2)]

    def sems(stage, i, t, d):
        return ssem.at[stage, i, t, d], rsem.at[stage, i, t, d]

    def hop(i, t, d):
        return send(so.at[lax.rem(i, 2), t, torus.step(1 - t, 2), d], rl.at[i, t, d],
                    sems(0, i, t, d), torus.near(1 - t, 1 - 2 * d))

    def whole(i, t, d, by):
        return send(so.at[lax.rem(i, 2), t, torus.step(1 - t, 1 - 2 * d)], ro.at[i, t, torus.step(1 - t, by)],
                    sems(1, i, t, d), torus.near(1 - t, 1 - 2 * d))

    def hop_on(i, t, d, by):
        return send(rl.at[i, t, d], ro.at[i, t, torus.step(1 - t, by), d],
                    sems(2, i, t, d), torus.near(1 - t, 1 - 2 * d))

    def own(i, t):
        return pltpu.make_async_copy(so.at[lax.rem(i, 2), t, at[1 - t]], ro.at[i, t, at[1 - t]],
                                     osem.at[lax.rem(i, 2), t])

    def far(i, t, d):
        return send(sh2.at[lax.rem(i, 2), t, d], rh2.at[i, t, d], sems(3, i, t, d), torus.near(t, 1 - 2 * d))

    def final(i, t, d):
        return send(sf2.at[lax.rem(i, 2), t, d], rf2.at[i, t, d], sems(4, i, t, d), torus.near(t, 1 - 2 * d))

    @pl.when((p == 0) & (e == 0))
    def _():
        load = pltpu.make_async_copy(w2_hbm, w2, wsem)
        load.start()
        greet([torus.near(axis, by) for axis in range(2) for by in (1, -1)])
        load.wait()

    @pl.when((e == 0) & (p >= 2) & (p < pairs + 2))
    def _():
        i = p - 2
        for t, d in ways:
            hop(i, t, d).wait_send()
            whole(i, t, d, 0).wait_send()
        for t in range(2):
            own(i, t).wait()

    @pl.when(p < pairs)
    def _():
        out = jnp.dot(h_ref[0], wd_ref[0], preferred_element_type=F32)
        rows = pl.ds(pl.multiple_of(e * 2 * slots, 2 * slots), 2 * slots)
        slot = lax.rem(p, 2)
        for k in range(side):
            for q in range(side // 2):
                a = (k * side + 2 * q) * slots
                so[slot, 0, k, q, rows] = out[a:a + 2 * slots, :hw].astype(BF16)
                b = [(i * side + k) * slots for i in (2 * q, 2 * q + 1)]
                so[slot, 1, k, q, rows] = jnp.concatenate(
                    [out[b[0]:b[0] + slots, hw:], out[b[1]:b[1] + slots, hw:]], axis=0).astype(BF16)

    @pl.when((p < pairs) & (e == experts - 1))
    def _():
        for t, d in ways:
            hop(p, t, d).start()
        for t, d in ways:
            whole(p, t, d, 0).start()
        for t in range(2):
            own(p, t).start()

    @pl.when((e == experts - 1) & (p >= 1) & (p < pairs + 1))
    def _():
        i = p - 1
        for t, d in ways:
            hop(i, t, d).wait_recv()
            hop_on(i, t, d, 2 * d - 1).start()

    @pl.when((e == experts - 1) & (p >= 2) & (p < pairs + 2))
    def _():
        i = p - 2
        for t, d in ways:
            whole(i, t, d, 2 * d - 1).wait_recv()
            hop_on(i, t, d, 2).wait_recv()

        @pl.when(i >= 2)
        def _():
            for t, d in ways:
                far(i - 2, t, d).wait_send()

        for t in range(2):
            for q in range(side // 2):
                total = jnp.dot(w2[(t * side) * 2 + q], ro[i, t, 0, q], preferred_element_type=F32)
                for j in range(1, side):
                    total += jnp.dot(w2[(t * side + j) * 2 + q], ro[i, t, j, q], preferred_element_type=F32)
                for k in range(2):
                    keep[lax.rem(i, 3), t, 2 * q + k] = total[k * tokens:(k + 1) * tokens]
        for t, d in ways:
            mine = keep.at[lax.rem(i, 3), t, torus.step(t, 2)]
            sh2[lax.rem(i, 2), t, d] = mine[halves[d], :].astype(BF16)
        for t, d in ways:
            far(i, t, d).start()

    @pl.when((e == experts - 1) & (p >= 3) & (p < pairs + 3))
    def _():
        i = p - 3
        for t, d in ways:
            far(i, t, d).wait_recv()

        @pl.when(i >= 2)
        def _():
            for t, d in ways:
                final(i - 2, t, d).wait_send()

        for t, d in ways:
            mine = keep.at[lax.rem(i, 3), t, torus.step(t, 1 - 2 * d)]
            there = rh2[i, t, d].astype(F32)
            sf2[lax.rem(i, 2), t, d, halves[d]] = (mine[halves[d], :] + there).astype(BF16)
            sf2[lax.rem(i, 2), t, d, halves[1 - d]] = mine[halves[1 - d], :].astype(BF16)
        for t, d in ways:
            final(i, t, d).start()

    @pl.when((e == experts - 1) & (p >= 4))
    def _():
        i = p - 4
        for t, d in ways:
            final(i, t, d).wait_recv()
        for t in range(2):
            y_ref[:, pl.ds(t * hw, hw)] = (
                keep[lax.rem(i, 3), t, at[t]] + rf2[i, t, 0].astype(F32)
                + rf2[i, t, 1].astype(F32)).astype(y_ref.dtype)

    @pl.when((e == experts - 1) & (p == pairs + 3))
    def _():
        for i in range(pairs):
            for t, d in ways:
                hop_on(i, t, d, 2 * d - 1).wait_send()
        for i in range(max(0, pairs - 2), pairs):
            for t, d in ways:
                far(i, t, d).wait_send()
                final(i, t, d).wait_send()


def solution(mesh, wide_in=WIDE_IN, wide_out=WIDE_OUT, limit=VMEM):
    n = mesh.shape["ep"]
    side = math.isqrt(n)
    dma = pltpu.SemaphoreType.DMA

    def step(x, expert, slot, gate, wg, wu, wd):
        x, expert, slot, gate = x[0, 0], expert[0, 0], slot[0, 0], gate[0, 0]
        tokens, d = x.shape
        top = expert.shape[1]
        local, _, ff = wg.shape
        slots = 5 * tokens * top // (4 * local * n)
        rows, tall = local * slots, n * slots
        big = n * local * slots
        code = jnp.where(slot < slots, expert * slots + slot, -4 * big).astype(F32)
        meta = jnp.concatenate([code.T, gate.T], axis=0)
        r = jnp.arange(2 * rows, dtype=jnp.int32)
        kind2 = r // (2 * slots) * slots + r % slots + (r // slots % 2) * 2 * big
        kind2 = jnp.broadcast_to(kind2.astype(F32)[:, None], (2 * rows, 128))
        kind = jnp.broadcast_to(jnp.arange(rows, dtype=jnp.int32).astype(F32)[:, None], (rows, 128))

        chunks, hw = d // wide_in, wide_in
        any_ = pl.BlockSpec(memory_space=pl.ANY)
        weight = pl.BlockSpec((1, wide_in, ff), lambda c, e: (e, c, 0))
        line = side * slots

        def all_of(v):
            return pl.BlockSpec(v.shape, lambda c, e: (0, 0))

        h, w2, _, _ = pl.pallas_call(
            functools.partial(gather_kernel, side, chunks, top, slots),
            grid=(chunks, local),
            in_specs=[all_of(meta), all_of(kind), all_of(kind2), any_, weight, weight],
            out_specs=[any_, any_, any_, any_],
            out_shape=[jax.ShapeDtypeStruct((local, side, line, ff), BF16),
                       jax.ShapeDtypeStruct((4 * side, 2 * tokens, 2 * rows), BF16),
                       jax.ShapeDtypeStruct((chunks, local, side, line, hw), BF16),
                       jax.ShapeDtypeStruct((chunks, 2, local // 2, line, hw), BF16)],
            scratch_shapes=[
                pltpu.VMEM((local, tall, ff), F32), pltpu.VMEM((local, tall, ff), F32),
                pltpu.VMEM((chunks, side, tokens, hw), BF16),
                pltpu.VMEM((local, side, line, hw), BF16),
                pltpu.VMEM((4, side, local, line, hw), BF16),
                pltpu.VMEM((2, side, side, rows, tokens), BF16),
                pltpu.VMEM((2 * tokens, 2 * rows), BF16),
                pltpu.VMEM((2, side, 2 * top, tokens), F32),
                dma((5, chunks, 2)), dma((5, chunks, 2)), dma((2, side)), dma((2, side)),
                dma((chunks,)), dma((local,)), dma((4,)), dma((ff // math.gcd(ff, wide_in),)), dma],
            compiler_params=pltpu.CompilerParams(
                collective_id=0, has_side_effects=True, vmem_limit_bytes=limit,
                dimension_semantics=("arbitrary", "arbitrary")),
        )(meta, kind, kind2, x, wg, wu)

        pairs, hw = d // wide_out, wide_out // 2
        half = tokens // 2
        y = pl.pallas_call(
            functools.partial(scatter_kernel, side, pairs, slots),
            grid=(pairs + 4, local),
            in_specs=[pl.BlockSpec((1, tall, ff), lambda p, e: (jnp.where(p < pairs, e, local - 1), 0, 0)),
                      pl.BlockSpec((1, ff, wide_out), lambda p, e: (
                          jnp.where(p < pairs, e, local - 1), 0, jnp.minimum(p, pairs - 1))), any_],
            out_specs=pl.BlockSpec((tokens, wide_out), lambda p, e: (0, jnp.maximum(p - 4, 0))),
            out_shape=jax.ShapeDtypeStruct((tokens, d), BF16),
            scratch_shapes=[
                pltpu.VMEM((4 * side, 2 * tokens, 2 * rows), BF16),
                pltpu.VMEM((2, 2, side, side // 2, 2 * rows, hw), BF16),
                pltpu.VMEM((pairs, 2, side, side // 2, 2 * rows, hw), BF16),
                pltpu.VMEM((pairs, 2, 2, 2 * rows, hw), BF16),
                pltpu.VMEM((3, 2, side, tokens, hw), F32),
                pltpu.VMEM((2, 2, 2, half, hw), BF16), pltpu.VMEM((2, 2, 2, tokens, hw), BF16),
                pltpu.VMEM((pairs, 2, 2, half, hw), BF16), pltpu.VMEM((pairs, 2, 2, tokens, hw), BF16),
                dma((5, pairs, 2, 2)), dma((5, pairs, 2, 2)), dma((2, 2)), dma],
            compiler_params=pltpu.CompilerParams(
                collective_id=1, has_side_effects=True, vmem_limit_bytes=limit,
                dimension_semantics=("arbitrary", "arbitrary")),
        )(h.reshape(local, tall, ff), wd, w2)
        return y[None, None]

    return jax.shard_map(
        step, mesh=mesh, in_specs=(P("dp", "ep"),) * 4 + (P("ep"),) * 3,
        out_specs=P("dp", "ep"), check_vma=False)
```

```python
import functools
import math

import jax
import jax.numpy as jnp
import numpy as np
from jax import lax
from jax.experimental import pallas as pl
from jax.experimental.pallas import tpu as pltpu
from jax.sharding import PartitionSpec as P

F32, BF16 = jnp.float32, jnp.bfloat16
WIDE_IN = 512
WIDE_OUT = 512
VMEM = 66_900_000


class Torus:
    def __init__(self, side):
        self.side = side
        self.me = lax.axis_index("ep")
        self.at = (self.me // side, self.me % side)

    def step(self, axis, by):
        return (self.at[axis] + by + self.side) % self.side

    def near(self, axis, by):
        place = list(self.at)
        place[axis] = self.step(axis, by)
        return place[0] * self.side + place[1]


def send(src, dst, sems, device):
    return pltpu.make_async_remote_copy(
        src_ref=src, dst_ref=dst, send_sem=sems[0], recv_sem=sems[1],
        device_id={"ep": device}, device_id_type=pl.DeviceIdType.MESH)


def greet(devices):
    barrier = pltpu.get_barrier_semaphore()
    for d in devices:
        pl.semaphore_signal(barrier, inc=1, device_id={"ep": d}, device_id_type=pl.DeviceIdType.MESH)
    pl.semaphore_wait(barrier, len(devices))


def spot(torus, t, j):
    return torus.at[0] * torus.side + j if t == 0 else j * torus.side + torus.at[1]


def gather_kernel(side, chunks, top, slots, meta_ref, row_ref, row2_ref, x_ref, wg_ref, wu_ref,
                  h_ref, w2_ref, zall, relay,
                  acc_g, acc_u, xl, zb, zs, d2, stage, meta,
                  ssem, rsem, msend, mrecv, lsem, zsem, osem, hsem, wsem):
    c, e = pl.program_id(0), pl.program_id(1)
    experts = pl.num_programs(1)
    local = zb.shape[0]
    tokens, hw = xl.shape[2:]
    torus = Torus(side)
    at = torus.at
    halves = (pl.ds(0, tokens // 2), pl.ds(tokens // 2, tokens // 2))
    parts = (pl.ds(0, local // 2), pl.ds(local // 2, local // 2))
    depth = zs.shape[0]
    step_of, last = c * experts + e, chunks - 1

    def sems(stage, k, d):
        return ssem.at[stage, k, d], rsem.at[stage, k, d]

    def first(k, t, d, by):
        b = xl.at[k, torus.step(t, by)]
        return send(b, b, sems(0, k, d), torus.near(t, 1 - 2 * d))

    def first_on(k, t, d, by):
        b = xl.at[k, torus.step(t, by), halves[d]]
        return send(b, b, sems(1, k, d), torus.near(t, 1 - 2 * d))

    def whole(k, t, d, by):
        return send(zs.at[lax.rem(k, depth), torus.step(1 - t, 1 - 2 * d)], zall.at[k, :, torus.step(1 - t, by)],
                    sems(2, k, d), torus.near(1 - t, 1 - 2 * d))

    def hop(k, t, d):
        return send(zs.at[lax.rem(k, depth), torus.step(1 - t, 2), parts[d]], relay.at[k, d],
                    sems(3, k, d), torus.near(1 - t, 1 - 2 * d))

    def hop_on(k, t, d, by):
        return send(relay.at[k, d], zall.at[k, parts[d], torus.step(1 - t, by)],
                    sems(4, k, d), torus.near(1 - t, 1 - 2 * d))

    def own(k, t):
        return pltpu.make_async_copy(zs.at[lax.rem(k, depth), at[1 - t]], zall.at[k, :, at[1 - t]],
                                     osem.at[lax.rem(k, depth)])

    def tell(axis, by, where):
        return send(meta_ref, meta.at[axis, torus.step(axis, where)],
                    (msend.at[axis, by], mrecv.at[axis, by]), torus.near(axis, by))

    def dispatch(k, t):
        slot = lax.rem(k, depth)
        for d in range(2):
            first_on(k, t, d, 2).wait_recv()

        @pl.when(k >= depth)
        def _():
            for d in range(2):
                hop(k - depth, t, d).wait_send()
                whole(k - depth, t, d, 0).wait_send()

        for j in range(side):
            for q in range(side // 2):
                got = [jnp.dot(d2[t, j, 2 * q + i], xl[k, 2 * q + i], preferred_element_type=F32) for i in range(2)]
                for m in range(local):
                    rows = slice(m * slots, (m + 1) * slots)
                    zs[slot, j, m, q * 2 * slots:(q + 1) * 2 * slots] = (
                        jnp.concatenate([got[0][rows], got[1][rows]], axis=0).astype(BF16))
        for d in range(2):
            hop(k, t, d).start()
        for d in range(2):
            whole(k, t, d, 0).start()
        own(k, t).start()

    def give(k, t):
        for d in range(2):
            first(k, t, d, 0).start()

    def hand_on(k, t):
        for d in range(2):
            first(k, t, d, 2 * d - 1).wait_recv()
            first_on(k, t, d, 2 * d - 1).start()

    def pass_on(k, t):
        for d in range(2):
            hop(k, t, d).wait_recv()
            hop_on(k, t, d, 2 * d - 1).start()

    @pl.when(step_of == 0)
    def _():
        loads = [pltpu.make_async_copy(x_ref.at[:, pl.ds(k * hw, hw)], xl.at[k, at[k % 2]], lsem.at[k])
                 for k in range(chunks)]
        for copy in loads:
            copy.start()
        greet([torus.near(axis, by) for axis in range(2) for by in range(1, side)])
        for axis in range(2):
            for by in range(1, side):
                tell(axis, by, 0).start()
        early = min(6, chunks)
        for k in range(chunks):
            loads[k].wait()
            if k < early:
                give(k, k % 2)
        for axis in range(2):
            meta[axis, at[axis]] = meta_ref[...]
        for axis in range(2):
            for by in range(1, side):
                tell(axis, by, -by).wait_recv()

        def build(t, i):
            @pl.loop(0, side)
            def _(j):
                code = meta[t, i][:top]
                row = row_ref[:, :1] + (spot(torus, t, j) * local * slots).astype(F32)
                hot = jnp.zeros((row.shape[0], tokens), F32)
                for m in range(top):
                    hot = jnp.where(code[m:m + 1] == row, 1.0, hot)
                d2[t, j, i] = hot.astype(BF16)

        todo = [(t, i) for t in range(2) for i in range(side)]
        for k in range(early):
            hand_on(k, k % 2)
            for t, i in todo[k * len(todo) // early:(k + 1) * len(todo) // early]:
                build(t, i)
        dispatch(0, 0)
        dispatch(1, 1)
        pass_on(0, 0)
        pass_on(1, 1)
        for k in range(early, chunks):
            give(k, k % 2)
        dispatch(2, 0)

    @pl.when((c == 1) & (e == 0))
    def _():
        for k in range(min(6, chunks), chunks):
            hand_on(k, k % 2)

    @pl.when(e == 0)
    def _():
        for t in range(2):
            @pl.when((c + 3 < chunks) & (lax.rem(c, 2) == 1 - t))
            def _():
                dispatch(c + 3, t)

        for t in range(2):
            @pl.when((c + 2 < chunks) & (lax.rem(c, 2) == t))
            def _():
                pass_on(c + 2, t)


            @pl.when(lax.rem(c, 2) == t)
            def _():
                for d in range(2):
                    whole(c, t, d, 2 * d - 1).wait_recv()
                    hop_on(c, t, d, 2).wait_recv()
                own(c, t).wait()
        for m in range(local):
            pltpu.make_async_copy(zall.at[c, m], zb.at[m], zsem.at[m]).start()

    @pl.when((step_of >= 8) & (step_of < 8 + 4 * side))
    def _():
        m = step_of - 8
        t, j, q = m // (2 * side), m // 2 % side, m % 2
        m0, m1 = meta[t, 2 * q], meta[t, 2 * q + 1]
        far = jnp.float32(2 * side * side * local * slots)
        code = jnp.concatenate([m0[:top], m1[:top] + far], axis=1)
        gate = jnp.concatenate([m0[top:], m1[top:]], axis=1)
        device = jnp.where(t == 0, at[0] * side + j, j * side + at[1])
        row = row2_ref[:, :1] + (device * local * slots).astype(F32)
        weight = jnp.zeros((row.shape[0], 2 * tokens), F32)
        for k in range(top):
            weight = jnp.where(code[k:k + 1] == row, gate[k:k + 1], weight)

        @pl.when(m > 0)
        def _():
            pltpu.make_async_copy(stage, w2_ref.at[m - 1], wsem).wait()

        stage[...] = weight.T.astype(BF16)
        pltpu.make_async_copy(stage, w2_ref.at[m], wsem).start()

    pltpu.make_async_copy(zall.at[c, e], zb.at[e], zsem.at[e]).wait()
    rows, ff = acc_g.shape[1:]
    tile = math.gcd(ff, hw)

    def products(o):
        cols = pl.ds(o, tile)
        zed = zb[e].reshape(rows, hw)
        return (cols, jnp.dot(zed, wg_ref[0, :, cols], preferred_element_type=F32),
                jnp.dot(zed, wu_ref[0, :, cols], preferred_element_type=F32))

    @pl.when(c == 0)
    def _():
        for o in range(0, ff, tile):
            cols, g, u = products(o)
            acc_g[e, :, cols] = g
            acc_u[e, :, cols] = u

    @pl.when((c > 0) & (lax.rem(c, 2) == 0))
    def _():
        for o in range(0, ff, tile):
            cols, g, u = products(o)
            acc_g[e, :, cols] += g
            acc_u[e, :, cols] += u

    @pl.when(lax.rem(c, 2) == 1)
    def _():
        for o in range(0, ff, tile):
            cols, g, u = products(o)
            for i in range(side):
                for j in range(side):
                    a, b = (i * side + j) * slots, (j * side + i) * slots
                    acc_g[e, a:a + slots, cols] += g[b:b + slots]
                    acc_u[e, a:a + slots, cols] += u[b:b + slots]

    @pl.when(c == last)
    def _():
        spare = (chunks - depth) % depth

        def put(m, o):
            return pltpu.make_async_copy(zs.at[spare, o // tile, :, :, pl.ds(0, tile)],
                                         h_ref.at[m, :, :, pl.ds(o, tile)], hsem.at[o // tile])

        @pl.when(e == 0)
        def _():
            for d in range(2):
                k, t = chunks - depth, (chunks - depth) % 2
                hop(k, t, d).wait_send()
                whole(k, t, d, 0).wait_send()

        for o in range(0, ff, tile):
            @pl.when(e > 0)
            def _():
                put(e - 1, o).wait()

            cols = pl.ds(o, tile)
            both = (jax.nn.silu(acc_g[e, :, cols]) * acc_u[e, :, cols]).astype(BF16)
            zs[spare, o // tile, :, :, pl.ds(0, tile)] = both.reshape(local, rows // local, tile)
            put(e, o).start()

        @pl.when(e == experts - 1)
        def _():
            for o in range(0, ff, tile):
                put(e, o).wait()

    @pl.when((c == last) & (e == experts - 1))
    def _():
        pltpu.make_async_copy(stage, w2_ref.at[4 * side - 1], wsem).wait()
        for k in range(chunks):
            for d in range(2):
                t = k % 2
                first(k, t, d, 0).wait_send()
                first_on(k, t, d, 2 * d - 1).wait_send()
                if k > chunks - depth:
                    hop(k, t, d).wait_send()
                    whole(k, t, d, 0).wait_send()
                hop_on(k, t, d, 2 * d - 1).wait_send()
        for axis in range(2):
            for by in range(1, side):
                tell(axis, by, 0).wait_send()


def scatter_kernel(side, pairs, slots, h_ref, wd_ref, w2_hbm, y_ref,
                   w2, so, ro, rl, keep, sh2, sf2, rh2, rf2, ssem, rsem, osem, wsem):
    p, e = pl.program_id(0), pl.program_id(1)
    experts = pl.num_programs(1)
    tokens, hw = keep.shape[-2:]
    half = tokens // 2
    torus = Torus(side)
    at = torus.at
    halves = (pl.ds(0, half), pl.ds(half, half))
    ways = [(t, d) for t in range(2) for d in range(2)]

    def sems(stage, i, t, d):
        return ssem.at[stage, i, t, d], rsem.at[stage, i, t, d]

    def hop(i, t, d):
        return send(so.at[lax.rem(i, 2), t, torus.step(1 - t, 2), d], rl.at[i, t, d],
                    sems(0, i, t, d), torus.near(1 - t, 1 - 2 * d))

    def whole(i, t, d, by):
        return send(so.at[lax.rem(i, 2), t, torus.step(1 - t, 1 - 2 * d)], ro.at[i, t, torus.step(1 - t, by)],
                    sems(1, i, t, d), torus.near(1 - t, 1 - 2 * d))

    def hop_on(i, t, d, by):
        return send(rl.at[i, t, d], ro.at[i, t, torus.step(1 - t, by), d],
                    sems(2, i, t, d), torus.near(1 - t, 1 - 2 * d))

    def own(i, t):
        return pltpu.make_async_copy(so.at[lax.rem(i, 2), t, at[1 - t]], ro.at[i, t, at[1 - t]],
                                     osem.at[lax.rem(i, 2), t])

    def far(i, t, d):
        return send(sh2.at[lax.rem(i, 2), t, d], rh2.at[i, t, d], sems(3, i, t, d), torus.near(t, 1 - 2 * d))

    def final(i, t, d):
        return send(sf2.at[lax.rem(i, 2), t, d], rf2.at[i, t, d], sems(4, i, t, d), torus.near(t, 1 - 2 * d))

    @pl.when((p == 0) & (e == 0))
    def _():
        pltpu.make_async_copy(w2_hbm, w2, wsem).start()
        greet([torus.near(axis, by) for axis in range(2) for by in (1, -1)])

    @pl.when((e == 0) & (p >= 2) & (p < pairs + 2))
    def _():
        i = p - 2
        for t, d in ways:
            hop(i, t, d).wait_send()
            whole(i, t, d, 0).wait_send()
        for t in range(2):
            own(i, t).wait()

    @pl.when(p < pairs)
    def _():
        out = jnp.dot(h_ref[0], wd_ref[0], preferred_element_type=F32)
        rows = pl.ds(pl.multiple_of(e * 2 * slots, 2 * slots), 2 * slots)
        slot = lax.rem(p, 2)
        for k in range(side):
            for q in range(side // 2):
                a = (k * side + 2 * q) * slots
                so[slot, 0, k, q, rows] = out[a:a + 2 * slots, :hw].astype(BF16)
                b = [(i * side + k) * slots for i in (2 * q, 2 * q + 1)]
                so[slot, 1, k, q, rows] = jnp.concatenate(
                    [out[b[0]:b[0] + slots, hw:], out[b[1]:b[1] + slots, hw:]], axis=0).astype(BF16)

    @pl.when((p < pairs) & (e == experts - 1))
    def _():
        for t, d in ways:
            hop(p, t, d).start()
        for t, d in ways:
            whole(p, t, d, 0).start()
        for t in range(2):
            own(p, t).start()

    @pl.when((e == experts - 1) & (p >= 1) & (p < pairs + 1))
    def _():
        i = p - 1
        for t, d in ways:
            hop(i, t, d).wait_recv()
            hop_on(i, t, d, 2 * d - 1).start()

    @pl.when((e == experts - 1) & (p >= 2) & (p < pairs + 2))
    def _():
        i = p - 2
        for t, d in ways:
            whole(i, t, d, 2 * d - 1).wait_recv()
            hop_on(i, t, d, 2).wait_recv()

        @pl.when(i == 0)
        def _():
            pltpu.make_async_copy(w2_hbm, w2, wsem).wait()

        @pl.when(i >= 2)
        def _():
            for t, d in ways:
                far(i - 2, t, d).wait_send()

        for t in range(2):
            for q in range(side // 2):
                total = jnp.dot(w2[(t * side) * 2 + q], ro[i, t, 0, q], preferred_element_type=F32)
                for j in range(1, side):
                    total += jnp.dot(w2[(t * side + j) * 2 + q], ro[i, t, j, q], preferred_element_type=F32)
                for k in range(2):
                    keep[lax.rem(i, 3), t, 2 * q + k] = total[k * tokens:(k + 1) * tokens]
        for t, d in ways:
            mine = keep.at[lax.rem(i, 3), t, torus.step(t, 2)]
            sh2[lax.rem(i, 2), t, d] = mine[halves[d], :].astype(BF16)
        for t, d in ways:
            far(i, t, d).start()

    @pl.when((e == experts - 1) & (p >= 3) & (p < pairs + 3))
    def _():
        i = p - 3
        for t, d in ways:
            far(i, t, d).wait_recv()

        @pl.when(i >= 2)
        def _():
            for t, d in ways:
                final(i - 2, t, d).wait_send()

        for t, d in ways:
            mine = keep.at[lax.rem(i, 3), t, torus.step(t, 1 - 2 * d)]
            there = rh2[i, t, d].astype(F32)
            sf2[lax.rem(i, 2), t, d, halves[d]] = (mine[halves[d], :] + there).astype(BF16)
            sf2[lax.rem(i, 2), t, d, halves[1 - d]] = mine[halves[1 - d], :].astype(BF16)
        for t, d in ways:
            final(i, t, d).start()

    @pl.when((e == experts - 1) & (p >= 4))
    def _():
        i = p - 4
        for t, d in ways:
            final(i, t, d).wait_recv()
        for t in range(2):
            y_ref[:, pl.ds(t * hw, hw)] = (
                keep[lax.rem(i, 3), t, at[t]] + rf2[i, t, 0].astype(F32)
                + rf2[i, t, 1].astype(F32)).astype(y_ref.dtype)

    @pl.when((e == experts - 1) & (p == pairs + 3))
    def _():
        for i in range(pairs):
            for t, d in ways:
                hop_on(i, t, d, 2 * d - 1).wait_send()
        for i in range(max(0, pairs - 2), pairs):
            for t, d in ways:
                far(i, t, d).wait_send()
                final(i, t, d).wait_send()


def solution(mesh, wide_in=WIDE_IN, wide_out=WIDE_OUT, limit=VMEM):
    n = mesh.shape["ep"]
    side = math.isqrt(n)
    dma = pltpu.SemaphoreType.DMA

    def step(x, expert, slot, gate, wg, wu, wd):
        x, expert, slot, gate = x[0, 0], expert[0, 0], slot[0, 0], gate[0, 0]
        tokens, d = x.shape
        top = expert.shape[1]
        local, _, ff = wg.shape
        slots = 5 * tokens * top // (4 * local * n)
        rows, tall = local * slots, n * slots
        big = n * local * slots
        code = jnp.where(slot < slots, expert * slots + slot, -4 * big).astype(F32)
        meta = jnp.concatenate([code.T, gate.T], axis=0)
        r = np.arange(2 * rows)
        kind2 = r // (2 * slots) * slots + r % slots + (r // slots % 2) * 2 * big
        kind2 = np.repeat(kind2.astype(np.float32)[:, None], 128, axis=1)
        kind = np.repeat(np.arange(rows, dtype=np.float32)[:, None], 128, axis=1)

        chunks, hw = d // wide_in, wide_in
        any_ = pl.BlockSpec(memory_space=pl.ANY)
        weight = pl.BlockSpec((1, wide_in, ff), lambda c, e: (e, c, 0))
        line = side * slots

        def all_of(v):
            return pl.BlockSpec(v.shape, lambda c, e: (0, 0))

        h, w2, _, _ = pl.pallas_call(
            functools.partial(gather_kernel, side, chunks, top, slots),
            grid=(chunks, local),
            in_specs=[all_of(meta), all_of(kind), all_of(kind2), any_, weight, weight],
            out_specs=[any_, any_, any_, any_],
            out_shape=[jax.ShapeDtypeStruct((local, side, line, ff), BF16),
                       jax.ShapeDtypeStruct((4 * side, 2 * tokens, 2 * rows), BF16),
                       jax.ShapeDtypeStruct((chunks, local, side, line, hw), BF16),
                       jax.ShapeDtypeStruct((chunks, 2, local // 2, line, hw), BF16)],
            scratch_shapes=[
                pltpu.VMEM((local, tall, ff), F32), pltpu.VMEM((local, tall, ff), F32),
                pltpu.VMEM((chunks, side, tokens, hw), BF16),
                pltpu.VMEM((local, side, line, hw), BF16),
                pltpu.VMEM((4, side, local, line, hw), BF16),
                pltpu.VMEM((2, side, side, rows, tokens), BF16),
                pltpu.VMEM((2 * tokens, 2 * rows), BF16),
                pltpu.VMEM((2, side, 2 * top, tokens), F32),
                dma((5, chunks, 2)), dma((5, chunks, 2)), dma((2, side)), dma((2, side)),
                dma((chunks,)), dma((local,)), dma((4,)), dma((ff // math.gcd(ff, wide_in),)), dma],
            compiler_params=pltpu.CompilerParams(
                collective_id=0, has_side_effects=True, vmem_limit_bytes=limit,
                dimension_semantics=("arbitrary", "arbitrary")),
        )(meta, kind, kind2, x, wg, wu)

        pairs, hw = d // wide_out, wide_out // 2
        half = tokens // 2
        y = pl.pallas_call(
            functools.partial(scatter_kernel, side, pairs, slots),
            grid=(pairs + 4, local),
            in_specs=[pl.BlockSpec((1, tall, ff), lambda p, e: (jnp.where(p < pairs, e, local - 1), 0, 0)),
                      pl.BlockSpec((1, ff, wide_out), lambda p, e: (
                          jnp.where(p < pairs, e, local - 1), 0, jnp.minimum(p, pairs - 1))), any_],
            out_specs=pl.BlockSpec((tokens, wide_out), lambda p, e: (0, jnp.maximum(p - 4, 0))),
            out_shape=jax.ShapeDtypeStruct((tokens, d), BF16),
            scratch_shapes=[
                pltpu.VMEM((4 * side, 2 * tokens, 2 * rows), BF16),
                pltpu.VMEM((2, 2, side, side // 2, 2 * rows, hw), BF16),
                pltpu.VMEM((pairs, 2, side, side // 2, 2 * rows, hw), BF16),
                pltpu.VMEM((pairs, 2, 2, 2 * rows, hw), BF16),
                pltpu.VMEM((3, 2, side, tokens, hw), F32),
                pltpu.VMEM((2, 2, 2, half, hw), BF16), pltpu.VMEM((2, 2, 2, tokens, hw), BF16),
                pltpu.VMEM((pairs, 2, 2, half, hw), BF16), pltpu.VMEM((pairs, 2, 2, tokens, hw), BF16),
                dma((5, pairs, 2, 2)), dma((5, pairs, 2, 2)), dma((2, 2)), dma],
            compiler_params=pltpu.CompilerParams(
                collective_id=1, has_side_effects=True, vmem_limit_bytes=limit,
                dimension_semantics=("arbitrary", "arbitrary")),
        )(h.reshape(local, tall, ff), wd, w2)
        return y[None, None]

    return jax.shard_map(
        step, mesh=mesh, in_specs=(P("dp", "ep"),) * 4 + (P("ep"),) * 3,
        out_specs=P("dp", "ep"), check_vma=False)
```
